32 devices in a mesh: dp: 16 (over z, x, core), tensor: 2 (over y).
Axes of the slice: x: 2, y: 2, z: 4, core: 2. Of those that a mesh axis runs over, the one named last changes fastest.
Arguments:
- inputs: bfloat16 [16, 256, 4096], P('dp', 'tensor'), may hold values from -40 to 40
- query_states: bfloat16 [16, 256, 3072], P('dp', None, 'tensor'), may hold values from -4.5 to 4.5
- key_states: bfloat16 [16, 256, 1024], P('dp', None, 'tensor'), may hold values from -4.5 to 4.5
- saved_value_states: bfloat16 [16, 256, 1024], P('dp', None, 'tensor'), may hold values from -4.5 to 4.5
- head_cotangent: bfloat16 [16, 256, 3072], P('dp', None, 'tensor'), may hold values from -40 to 40
- query_weight: bfloat16 [4096, 3072], P('dp', 'tensor'), may hold values from -0.09375 to 0.09375
- key_matrix: bfloat16 [4096, 1024], P('dp', 'tensor'), may hold values from -0.09375 to 0.09375
- value_matrix: bfloat16 [4096, 1024], P('dp', 'tensor'), may hold values from -0.09375 to 0.09375
- query_momentum: float32 [4096, 3072], P('dp', 'tensor'), may hold values from -6 to 6
- key_prior_momentum: float32 [4096, 1024], P('dp', 'tensor'), may hold values from -6 to 6
- value_prior_momentum: float32 [4096, 1024], P('dp', 'tensor'), may hold values from -6 to 6
Outputs:
- input_gradient: bfloat16 [16, 256, 4096], P('dp', 'tensor')
- query_velocity: float32 [4096, 3072], P('dp', 'tensor')
- key_velocity: float32 [4096, 1024], P('dp', 'tensor')
- value_velocity: float32 [4096, 1024], P('dp', 'tensor')
The draws below stay inside these ranges and needn't reach their ends.
All inputs are finite; a program needn't handle non-finite values.
Results may differ from the reference program's by a relative error of at most 0.019.
Values may be sent and summed in bfloat16 or wider, within the bound.
No kernel may reach another device: no remote copies, remote signals or barrier semaphores. Data moves between devices by JAX's collectives and lax.ppermute only.
A program may use at most 128 MiB of HBM per device.

```python
import math
import jax
import jax.numpy as jnp
from jax import lax

MODEL_FEATURES = 4096
QUERY_HEADS = 24
KEY_VALUE_HEADS = 8
HEAD_SIZE = 128
SEQUENCE_LENGTH = 256
SEQUENCE_COUNT = 16
N_TENSOR = 2


def column_scales(base_key, width, head_width):
    spread = jnp.exp(jax.random.uniform(base_key, (width,), jnp.float32, math.log(0.3), math.log(3.0)))
    position = (jnp.arange(width, dtype=jnp.int32) // head_width).astype(jnp.float32)
    last_index = max(width // head_width - 1, 1)
    rising = jnp.exp(math.log(3.0) * (position / last_index - 0.5))
    return (spread, rising)


def draw_scaled(base_key, array_shape, head_width):
    key_scale, key_noise = jax.random.split(base_key, 2)
    width = array_shape[-1]
    spread, rising = column_scales(key_scale, width, head_width)
    value_entries = jnp.clip(jax.random.normal(key_noise, array_shape, jnp.float32), -4.0, 4.0) * spread * rising
    return value_entries


def draw_inputs(key, part):
    return draw_scaled(jax.random.fold_in(key, 11), (SEQUENCE_COUNT, SEQUENCE_LENGTH, MODEL_FEATURES), 1).astype(jnp.bfloat16)


def draw_head_cotangent(key, part):
    return draw_scaled(jax.random.fold_in(key, 13), (SEQUENCE_COUNT, SEQUENCE_LENGTH, QUERY_HEADS * HEAD_SIZE), HEAD_SIZE).astype(jnp.bfloat16)


def draw_query_states(key, part):
    base_key = jax.random.fold_in(key, 17)
    array_shape = (SEQUENCE_COUNT, SEQUENCE_LENGTH, QUERY_HEADS, HEAD_SIZE)
    value_entries = jnp.clip(jax.random.normal(base_key, array_shape, jnp.float32), -4.5, 4.5)
    return value_entries.reshape(SEQUENCE_COUNT, SEQUENCE_LENGTH, QUERY_HEADS * HEAD_SIZE).astype(jnp.bfloat16)


def draw_key_states(key, part):
    base_key = jax.random.fold_in(key, 19)
    array_shape = (SEQUENCE_COUNT, SEQUENCE_LENGTH, KEY_VALUE_HEADS, HEAD_SIZE)
    value_entries = jnp.clip(jax.random.normal(base_key, array_shape, jnp.float32), -4.5, 4.5)
    return value_entries.reshape(SEQUENCE_COUNT, SEQUENCE_LENGTH, KEY_VALUE_HEADS * HEAD_SIZE).astype(jnp.bfloat16)


def block_levels(own_key, extent, cuts, low, top_value):
    gain, own = 1.0, jax.random.fold_in(own_key, 6)
    for dim, shards_of in cuts:
        draws = jnp.exp(jax.random.uniform(jax.random.fold_in(own, dim), (shards_of,), jnp.float32, low / len(cuts), top_value / len(cuts)))
        gain = gain * jnp.repeat(draws, extent[dim] // shards_of).reshape([-1 if axis == dim else 1 for axis in range(len(extent))])
    return gain


def scatter_about(rng, extent, deviation, limit, shards=(), kind=jnp.bfloat16):
    values = deviation * jax.random.normal(rng, extent, jnp.float32)
    if shards:
        values = values * block_levels(rng, extent, shards, -0.22, 0.18)
    return jnp.clip(values, -limit, limit).astype(kind)


def setup_inputs(seed: int = 0) -> dict:
    arg_keys = jax.random.split(jax.random.key(seed), 12)
    return {
        "inputs": draw_inputs(jax.random.fold_in(arg_keys[11], 71), 0),
        "query_states": draw_query_states(jax.random.fold_in(arg_keys[11], 71), 0),
        "key_states": draw_key_states(jax.random.fold_in(arg_keys[11], 71), 0),
        "saved_value_states": scatter_about(arg_keys[3], (SEQUENCE_COUNT, SEQUENCE_LENGTH, KEY_VALUE_HEADS * HEAD_SIZE), 1.0, 4.5, ((0, 16), (2, 2))),
        "head_cotangent": draw_head_cotangent(jax.random.fold_in(arg_keys[11], 71), 0),
        "query_weight": scatter_about(arg_keys[5], (MODEL_FEATURES, QUERY_HEADS * HEAD_SIZE), MODEL_FEATURES ** -0.5, 0.09375, ((0, 16), (1, 2))),
        "key_matrix": scatter_about(arg_keys[6], (MODEL_FEATURES, KEY_VALUE_HEADS * HEAD_SIZE), MODEL_FEATURES ** -0.5, 0.09375, ((0, 16), (1, 2))),
        "value_matrix": scatter_about(arg_keys[7], (MODEL_FEATURES, KEY_VALUE_HEADS * HEAD_SIZE), MODEL_FEATURES ** -0.5, 0.09375, ((0, 16), (1, 2))),
        "query_momentum": scatter_about(arg_keys[8], (MODEL_FEATURES, QUERY_HEADS * HEAD_SIZE), 1.0, 6.0, ((0, 16), (1, 2)), jnp.float32),
        "key_prior_momentum": scatter_about(arg_keys[9], (MODEL_FEATURES, KEY_VALUE_HEADS * HEAD_SIZE), 1.0, 6.0, ((0, 16), (1, 2)), jnp.float32),
        "value_prior_momentum": scatter_about(arg_keys[10], (MODEL_FEATURES, KEY_VALUE_HEADS * HEAD_SIZE), 1.0, 6.0, ((0, 16), (1, 2)), jnp.float32),
    }


def rounded(value_entries):
    return lax.optimization_barrier(value_entries.astype(jnp.bfloat16)).astype(jnp.float32)

def sequence_backward(sequence_queries, sequence_keys, sequence_values, sequence_cotangent):
    token_length = sequence_queries.shape[0]
    group_width = QUERY_HEADS // KEY_VALUE_HEADS
    scaling = 1.0 / math.sqrt(HEAD_SIZE)
    query_quad = sequence_queries.astype(jnp.float32).reshape(token_length, KEY_VALUE_HEADS, group_width, HEAD_SIZE)
    cotangent_quad = sequence_cotangent.astype(jnp.float32).reshape(token_length, KEY_VALUE_HEADS, group_width, HEAD_SIZE)
    key_triple = sequence_keys.astype(jnp.float32).reshape(token_length, KEY_VALUE_HEADS, HEAD_SIZE)
    value_triple = sequence_values.astype(jnp.float32).reshape(token_length, KEY_VALUE_HEADS, HEAD_SIZE)
    scores = jnp.einsum('ihgd,jhd->hgij', query_quad, key_triple) * scaling
    position = jnp.arange(token_length, dtype=jnp.int32)
    causal = position[:, None] >= position[None, :]
    scores = jnp.where(causal, scores, -jnp.inf)
    maximum = lax.optimization_barrier(jnp.max(scores, axis=-1, keepdims=True))
    exponent = jnp.exp(scores - maximum)
    softmax_rows = exponent / lax.optimization_barrier(jnp.sum(exponent, axis=-1, keepdims=True))
    softmax_reduced = rounded(softmax_rows)
    grad_softmax = jnp.einsum('ihgd,jhd->hgij', cotangent_quad, value_triple)
    row_delta = lax.optimization_barrier(jnp.sum(softmax_rows * grad_softmax, axis=-1, keepdims=True))
    score_gradient = rounded(softmax_rows * (grad_softmax - row_delta) * scaling)
    grad_query = jnp.einsum('hgij,jhd->ihgd', score_gradient, key_triple).astype(jnp.bfloat16).reshape(token_length, QUERY_HEADS * HEAD_SIZE)
    key_gradient = jnp.einsum('xfwo,wxfp->oxp', score_gradient, query_quad).astype(jnp.bfloat16).reshape(token_length, KEY_VALUE_HEADS * HEAD_SIZE)
    value_gradient = jnp.einsum('xfwo,wxfp->oxp', softmax_reduced, cotangent_quad).astype(jnp.bfloat16).reshape(token_length, KEY_VALUE_HEADS * HEAD_SIZE)
    return (grad_query, key_gradient, value_gradient)

def reference(inputs, query_states, key_states, saved_value_states, head_cotangent, query_weight, key_matrix, value_matrix, query_momentum, key_prior_momentum, value_prior_momentum):
    query_share = QUERY_HEADS * HEAD_SIZE // N_TENSOR
    paired_portion = KEY_VALUE_HEADS * HEAD_SIZE // N_TENSOR

    def one_sequence(running, sequence_slices):
        input_seq, sequence_queries, sequence_keys, sequence_values, sequence_cotangent = sequence_slices
        grad_query, key_gradient, value_gradient = sequence_backward(sequence_queries, sequence_keys, sequence_values, sequence_cotangent)
        summed = jnp.zeros((input_seq.shape[0], MODEL_FEATURES), jnp.float32)
        for block_index in range(N_TENSOR):
            query_span = slice(block_index * query_share, (block_index + 1) * query_share)
            pair_span = slice(block_index * paired_portion, (block_index + 1) * paired_portion)
            partial_value = jnp.dot(grad_query[:, query_span], query_weight[:, query_span].T, preferred_element_type=jnp.float32)
            partial_value = partial_value + jnp.dot(key_gradient[:, pair_span], key_matrix[:, pair_span].T, preferred_element_type=jnp.float32)
            partial_value = partial_value + jnp.dot(value_gradient[:, pair_span], value_matrix[:, pair_span].T, preferred_element_type=jnp.float32)
            summed = summed + rounded(partial_value)
        running_query, running_key, running_value = running
        input_trans = input_seq.T
        running_query = running_query + rounded(jnp.dot(input_trans, grad_query, preferred_element_type=jnp.float32))
        running_key = running_key + rounded(jnp.dot(input_trans, key_gradient, preferred_element_type=jnp.float32))
        running_value = running_value + rounded(jnp.dot(input_trans, value_gradient, preferred_element_type=jnp.float32))
        return ((running_query, running_key, running_value), summed.astype(jnp.bfloat16))
    initial_state = (jnp.zeros((MODEL_FEATURES, QUERY_HEADS * HEAD_SIZE), jnp.float32), jnp.zeros((MODEL_FEATURES, KEY_VALUE_HEADS * HEAD_SIZE), jnp.float32), jnp.zeros((MODEL_FEATURES, KEY_VALUE_HEADS * HEAD_SIZE), jnp.float32))
    sums, input_gradient = lax.scan(one_sequence, initial_state, (inputs, query_states, key_states, saved_value_states, head_cotangent))
    grad_w_query, grad_w_key, grad_w_value = sums
    squared_total = jnp.sum(grad_w_query * grad_w_query) + jnp.sum(grad_w_key * grad_w_key) + jnp.sum(grad_w_value * grad_w_value)
    root_mean_square = jnp.sqrt(squared_total / (MODEL_FEATURES * (QUERY_HEADS + 2 * KEY_VALUE_HEADS) * HEAD_SIZE))
    factor = 1.0 / jnp.maximum(root_mean_square, 1.0)
    query_velocity = 0.9 * query_momentum + factor * grad_w_query
    key_velocity = 0.9 * key_prior_momentum + factor * grad_w_key
    value_velocity = 0.9 * value_prior_momentum + factor * grad_w_value
    return (input_gradient, query_velocity, key_velocity, value_velocity)
```

```python
import math

import jax
import jax.numpy as jnp
from jax import lax
from jax.sharding import PartitionSpec as P

MODEL_FEATURES = 4096
QUERY_HEADS = 24
KEY_VALUE_HEADS = 8
HEAD_SIZE = 128
GROUP = 4


def heads_backward(query_rows, key_rows, value_rows, cotangent_rows):
    tokens = query_rows.shape[0]
    kv_heads = key_rows.shape[1] // HEAD_SIZE
    group = query_rows.shape[1] // HEAD_SIZE // kv_heads
    scaling = 1.0 / math.sqrt(HEAD_SIZE)
    query = query_rows.reshape(tokens, kv_heads, group, HEAD_SIZE)
    cotangent = cotangent_rows.reshape(tokens, kv_heads, group, HEAD_SIZE)
    key = key_rows.reshape(tokens, kv_heads, HEAD_SIZE)
    value = value_rows.reshape(tokens, kv_heads, HEAD_SIZE)
    f32 = jnp.float32
    block = min(tokens, 512)
    key_sums = jnp.zeros((tokens, kv_heads, HEAD_SIZE), f32)
    value_sums = jnp.zeros((tokens, kv_heads, HEAD_SIZE), f32)
    query_blocks = []
    for start in range(0, tokens, block):
        end = start + block
        q, g, k, v = query[start:end], cotangent[start:end], key[:end], value[:end]
        scores = jnp.einsum("ihgd,jhd->hgij", q, k, preferred_element_type=f32) * scaling
        row = start + lax.broadcasted_iota(jnp.int32, (block, end), 0)
        col = lax.broadcasted_iota(jnp.int32, (block, end), 1)
        scores = jnp.where(row >= col, scores, -jnp.inf)
        exponent = jnp.exp(scores - jnp.max(scores, axis=-1, keepdims=True))
        soft = exponent / jnp.sum(exponent, axis=-1, keepdims=True)
        low = soft.astype(jnp.bfloat16)
        grad_soft = jnp.einsum("ihgd,jhd->hgij", g, v, preferred_element_type=f32)
        delta = jnp.sum(soft * grad_soft, axis=-1, keepdims=True)
        grad_scores = (soft * (grad_soft - delta) * scaling).astype(jnp.bfloat16)
        query_blocks.append(
            jnp.einsum("hgij,jhd->ihgd", grad_scores, k, preferred_element_type=f32).astype(jnp.bfloat16)
        )
        key_sums = key_sums.at[:end].add(
            jnp.einsum("xfwo,wxfp->oxp", grad_scores, q, preferred_element_type=f32)
        )
        value_sums = value_sums.at[:end].add(
            jnp.einsum("xfwo,wxfp->oxp", low, g, preferred_element_type=f32)
        )
    return jnp.concatenate(
        [
            jnp.concatenate(query_blocks, axis=0).reshape(tokens, -1),
            key_sums.astype(jnp.bfloat16).reshape(tokens, -1),
            value_sums.astype(jnp.bfloat16).reshape(tokens, -1),
        ],
        axis=1,
    )


def pick(choices, index):
    result = choices[0]
    for j in range(1, len(choices)):
        result = jnp.where(index == j, choices[j], result)
    return result


def local_of(dp, nt):
    lines = dp // GROUP

    def line_shift(a, pairs):
        return lax.ppermute(a, "dp", [(i * GROUP + b, j * GROUP + b) for i, j in pairs for b in range(GROUP)])

    def xor_dp(a, m):
        return lax.ppermute(a, "dp", [(i, i ^ m) for i in range(dp)])

    def line_gather(a, z):
        right, left = {0: a}, {0: a}
        for k in range(1, lines):
            right[k] = line_shift(right[k - 1], [(i, i + 1) for i in range(k - 1, lines - 1)])
            left[k] = line_shift(left[k - 1], [(i, i - 1) for i in range(1, lines - k + 1)])
        return [a] + [jnp.where(z >= k, right[k], left[lines - k]) for k in range(1, lines)]

    def local(inputs, qs, ks, vs, dos, wq, wk, wv, mq, mk, mv):
        f32, bf = jnp.float32, jnp.bfloat16
        i = lax.axis_index("dp")
        t = lax.axis_index("tensor")
        z, x, c = i // GROUP, (i // 2) % 2, i % 2
        tok, features = inputs.shape[1], inputs.shape[2]
        seq = tok * nt
        width = features // lines
        rows = wq.shape[0]
        kv = ks.shape[2] // HEAD_SIZE
        pieces = 2 if kv % 2 == 0 else 1

        def cols(a, p):
            w = a.shape[-1] // pieces
            return a[..., p * w : (p + 1) * w]

        own = inputs[0]
        slots = []
        for k in range(lines):
            part = pick([own[:, j * width : (j + 1) * width] for j in range(lines)], (z + k) % lines)
            slots.append(part if k == 0 else line_shift(part, [(j, (j + k) % lines) for j in range(lines)]))
        mine = jnp.stack(slots)
        if nt == 2:
            other = lax.ppermute(mine, "tensor", [(0, 1), (1, 0)])
            first = jnp.where(t == 0, mine, other)
            second = jnp.where(t == 0, other, mine)
            tokens_in = jnp.concatenate([first[:, None], second[:, None]], axis=1)
        else:
            tokens_in = lax.all_gather(mine[:, None], "tensor", axis=1, tiled=True)
        tokens_in = tokens_in.reshape(lines * seq, width)

        w = jnp.concatenate([cols(a, p) for p in range(pieces) for a in (wq, wk, wv)], axis=1)
        w_other = xor_dp(w, 2)
        gathered, sums = [], []
        for p in range(pieces):
            grads = heads_backward(cols(qs[0], p), cols(ks[0], p), cols(vs[0], p), cols(dos[0], p))
            gathered.append(jnp.concatenate(line_gather(grads, z), axis=0))

        w_other, gathered[-1] = lax.optimization_barrier((w_other, gathered[-1]))
        upper = jnp.where(x == 0, w, w_other)
        lower = jnp.where(x == 0, w_other, w)
        upper_other, lower_other = xor_dp(upper, 1), xor_dp(lower, 1)
        quad = jnp.concatenate(
            [
                jnp.where(c == 0, upper, upper_other),
                jnp.where(c == 0, upper_other, upper),
                jnp.where(c == 0, lower, lower_other),
                jnp.where(c == 0, lower_other, lower),
            ],
            axis=0,
        )
        for p in range(pieces):
            part = lax.dot_general(
                tokens_in, gathered[p], (((0,), (0,)), ((), ())), preferred_element_type=f32
            ).astype(bf).reshape(2, 2, rows, -1)
            keep = jnp.where(c == 0, part[:, 0], part[:, 1])
            send = jnp.where(c == 0, part[:, 1], part[:, 0])
            half = (keep.astype(f32) + xor_dp(send, 1).astype(f32)).astype(bf)
            keep = jnp.where(x == 0, half[0], half[1])
            send = jnp.where(x == 0, half[1], half[0])
            sums.append(keep.astype(f32) + xor_dp(send, 2).astype(f32))

        total = sum(jnp.sum(s * s) for s in sums).reshape(1, 1)
        m = 1
        while m < dp:
            total = total + xor_dp(total, m)
            m *= 2
        m = 1
        while m < nt:
            total = total + lax.ppermute(total, "tensor", [(j, j ^ m) for j in range(nt)])
            m *= 2
        count = MODEL_FEATURES * (QUERY_HEADS + 2 * KEY_VALUE_HEADS) * HEAD_SIZE
        factor = 1.0 / jnp.maximum(jnp.sqrt(total / count), 1.0)
        a, b = wq.shape[1] // pieces, wk.shape[1] // pieces
        gq = jnp.concatenate([s[:, :a] for s in sums], axis=1)
        gk = jnp.concatenate([s[:, a : a + b] for s in sums], axis=1)
        gv = jnp.concatenate([s[:, a + b :] for s in sums], axis=1)
        velocities = tuple(0.9 * m0 + factor * g for m0, g in ((mq, gq), (mk, gk), (mv, gv)))

        pw = quad.shape[1] // pieces
        product = sum(
            lax.dot_general(
                gathered[p], quad[:, p * pw : (p + 1) * pw], (((1,), (1,)), ((), ())),
                preferred_element_type=f32,
            )
            for p in range(pieces)
        ).astype(bf).reshape(lines, nt, tok, width)
        blocks = []
        for k in range(lines):
            if nt == 2:
                keep = jnp.where(t == 0, product[k, 0], product[k, 1])
                send = jnp.where(t == 0, product[k, 1], product[k, 0])
                got = lax.ppermute(send, "tensor", [(0, 1), (1, 0)])
                block = (keep.astype(f32) + got.astype(f32)).astype(bf)
            else:
                block = lax.psum_scatter(product[k], "tensor", scatter_dimension=0, tiled=False)
            if k:
                block = line_shift(block, [(j, (j - k) % lines) for j in range(lines)])
            blocks.append(block)
        out = jnp.concatenate([pick(blocks, (j - z) % lines) for j in range(lines)], axis=1)
        return (out[None],) + velocities

    return local


def solution(mesh):
    rows = P("dp", "tensor")
    heads = P("dp", None, "tensor")
    tokens = P("dp", "tensor", None)
    return jax.shard_map(
        local_of(mesh.shape["dp"], mesh.shape["tensor"]),
        mesh=mesh,
        in_specs=(tokens, heads, heads, heads, heads) + (rows,) * 6,
        out_specs=(tokens, rows, rows, rows),
        check_vma=False,
    )
```
